32 devices in a mesh: dp: 1 (over z), sp: 32 (over x, y, core).
Axes of the slice: x: 4, y: 4, z: 1, core: 2. Of those that a mesh axis runs over, the one named last changes fastest.
The devices are a block of a 4x4x8 slice.
Arguments:
- q: bfloat16 [32, 8, 256], P('dp')
- k: bfloat16 [32, 8192, 8, 256], P('dp', 'sp')
- v: bfloat16 [32, 8192, 8, 256], P('dp', 'sp')
Outputs:
- q: bfloat16 [32, 8, 256], P('dp')
All inputs are finite; a program needn't handle non-finite values.
Results may differ from the reference program's by a relative error of at most 0.012.
Values are sent between devices in bfloat16 or wider.
A program may use at most 768 MiB of HBM per device.

```python
import jax
import jax.numpy as jnp

BATCH = 32
CACHE = 8192
HEADS = 8
KV_HEADS = 8
HEAD = 256


def setup_inputs(seed: int = 0, part: int = 0) -> dict:
    kq, kk, kv = (jax.random.fold_in(k, part) for k in jax.random.split(jax.random.key(seed), 3))
    return {
        "q": (3 * jax.random.normal(kq, (BATCH, HEADS, HEAD), jnp.float32)).astype(jnp.bfloat16),
        "k": jax.random.normal(kk, (BATCH, CACHE, KV_HEADS, HEAD), jnp.float32).astype(jnp.bfloat16),
        "v": jax.random.normal(kv, (BATCH, CACHE, KV_HEADS, HEAD), jnp.float32).astype(jnp.bfloat16),
    }


def einsum(form, a, b):
    return jnp.einsum(form, a.astype(jnp.float32), b.astype(jnp.float32))


def reference(q, k, v):
    grouped = q.reshape(BATCH, KV_HEADS, -1, HEAD)
    scores = einsum("bgsd,bugd->bgsu", grouped, k) * HEAD**-0.5
    weights = jax.nn.softmax(scores, -1).astype(jnp.bfloat16)
    return einsum("bgsu,bugd->bgsd", weights, v).astype(jnp.bfloat16).reshape(BATCH, HEADS, HEAD)
```

```python
import functools
import math

import jax
import jax.numpy as jnp
from jax import lax
from jax.experimental import pallas as pl
from jax.experimental.pallas import tpu as pltpu
from jax.sharding import PartitionSpec as P

MESH = pl.DeviceIdType.MESH
GROUP = 2
SLOTS = 8
LAG1 = 3
LAG2 = 6


def kernel(inner, outer, heads, q_ref, k_hbm, v_hbm, o_ref, kbuf, vbuf, parts1, stats1, parts2, stats2, ksem, vsem, sent1, sent2, got1, got2, statsent1, statsent2, statgot1, statgot2):
    steps, _, rows, head = parts1.shape
    tokens = k_hbm.shape[1]
    me, group = lax.axis_index("sp"), lax.axis_index("dp")
    row, col = lax.div(me, inner), lax.rem(me, inner)
    peers1 = [row * inner + lax.rem(col + j, inner) for j in range(1, inner)]
    peers2 = [lax.rem(row + j, outer) * inner + col for j in range(1, outer)]

    def fetch(hbm, buf, sem, i):
        slot = lax.rem(i, SLOTS)
        return pltpu.make_async_copy(hbm.at[pl.ds(i * GROUP, GROUP)], buf.at[slot], sem.at[slot])

    def prefetch(i, _):
        fetch(k_hbm, kbuf, ksem, i).start()
        fetch(v_hbm, vbuf, vsem, i).start()
        return 0

    lax.fori_loop(0, min(SLOTS, steps), prefetch, 0)

    barrier = pltpu.get_barrier_semaphore()
    for peer in peers1 + peers2:
        pl.semaphore_signal(barrier, inc=1, device_id=(group, peer), device_id_type=MESH)

    own = lax.rem(lax.broadcasted_iota(jnp.int32, (heads, tokens), 1), heads) == lax.broadcasted_iota(jnp.int32, (heads, tokens), 0)
    eye = lax.broadcasted_iota(jnp.int32, (rows, 128), 1) == lax.broadcasted_iota(jnp.int32, (rows, 128), 0)

    def across(column):
        return jnp.sum(jnp.where(eye, column, 0.0), 0, keepdims=True)

    def down(line):
        return jnp.sum(jnp.where(eye, line, 0.0), 1, keepdims=True)

    def send(parts, stats, i, mine, peers, sent, got, statsent, statgot):
        for ref, out, into in ((parts, sent, got), (stats, statsent, statgot)):
            for peer in peers:
                pltpu.make_async_remote_copy(
                    src_ref=ref.at[i, mine], dst_ref=ref.at[i, mine], send_sem=out, recv_sem=into.at[i], device_id=(group, peer), device_id_type=MESH
                ).start()

    def arrived(ref, i, count, sem):
        part = ref.at[i, pl.ds(0, count)]
        pltpu.make_async_copy(part, part, sem.at[i]).wait()

    def attend(i):
        slot = lax.rem(i, SLOTS)
        fetch(k_hbm, kbuf, ksem, i).wait()
        scores = []
        for g in range(GROUP):
            scores.append(lax.dot_general(q_ref[i * GROUP + g], kbuf[slot, g], (((1,), (1,)), ((), ())), preferred_element_type=jnp.float32))
        highs, totals, weights = [], [], []
        for g in range(GROUP):
            s = jnp.where(own, scores[g] * head**-0.5, -jnp.inf)
            high = jnp.max(s, 1, keepdims=True)
            w = jnp.exp(s - high)
            highs.append(high)
            totals.append(jnp.sum(w, 1, keepdims=True))
            weights.append(w.astype(jnp.bfloat16))
        fetch(v_hbm, vbuf, vsem, i).wait()
        seen = [jnp.dot(weights[g], vbuf[slot, g], preferred_element_type=jnp.float32) for g in range(GROUP)]
        parts1[i, col] = jnp.concatenate(seen, 0).astype(jnp.bfloat16)
        stats1[i, col] = jnp.concatenate([across(jnp.concatenate(highs, 0)), across(jnp.concatenate(totals, 0))], 0)

    def merge(parts, stats, i, count):
        high = stats[i, :, 0, :]
        top = jnp.max(high, 0, keepdims=True)
        scale = jnp.exp(high - top)
        total = jnp.sum(stats[i, :, 1, :] * scale, 0, keepdims=True)
        seen = sum(down(scale[s : s + 1]) * parts[i, s].astype(jnp.float32) for s in range(count))
        return seen, total, top

    def first(i):
        arrived(parts1, i, inner - 1, got1)
        arrived(stats1, i, inner - 1, statgot1)
        seen, total, top = merge(parts1, stats1, i, inner)
        parts2[i, row] = seen.astype(jnp.bfloat16)
        stats2[i, row] = jnp.concatenate([top, total], 0)
        send(parts2, stats2, i, row, peers2, sent2, got2, statsent2, statgot2)

    def second(i):
        arrived(parts2, i, outer - 1, got2)
        arrived(stats2, i, outer - 1, statgot2)
        seen, total, _ = merge(parts2, stats2, i, outer)
        o_ref[pl.ds(i * rows, rows), :] = (seen / down(total)).astype(o_ref.dtype)

    def step(i, _):
        attend(i)

        @pl.when(i == 0)
        def _():
            pl.semaphore_wait(barrier, inner + outer - 2)

        send(parts1, stats1, i, col, peers1, sent1, got1, statsent1, statgot1)

        @pl.when(i + SLOTS < steps)
        def _():
            prefetch(i + SLOTS, 0)

        @pl.when(i >= LAG1)
        def _():
            first(i - LAG1)

        @pl.when(i >= LAG2)
        def _():
            second(i - LAG2)

        return 0

    lax.fori_loop(0, steps, step, 0)

    def drain(i, _):
        @pl.when(i - LAG1 < steps)
        def _():
            first(i - LAG1)

        second(i - LAG2)
        return 0

    lax.fori_loop(steps, steps + LAG2, drain, 0)

    for ref, count, sem in ((parts1, inner - 1, sent1), (parts2, outer - 1, sent2), (stats1, inner - 1, statsent1), (stats2, outer - 1, statsent2)):
        part = ref.at[:, pl.ds(0, count)]
        pltpu.make_async_copy(part, part, sem).wait()


def solution(mesh):
    n = mesh.shape["sp"]
    outer = math.isqrt(n // 2)
    inner = n // outer

    def step(q, k, v):
        batch, tokens, heads, head = k.shape
        steps, rows = batch // GROUP, GROUP * heads
        k, v = (a.reshape(batch, tokens * heads, head) for a in (k, v))
        out = pl.pallas_call(
            functools.partial(kernel, inner, outer, heads),
            out_shape=jax.ShapeDtypeStruct((batch * heads, head), q.dtype),
            in_specs=[pl.BlockSpec(memory_space=pltpu.VMEM), pl.BlockSpec(memory_space=pl.ANY), pl.BlockSpec(memory_space=pl.ANY)],
            out_specs=pl.BlockSpec(memory_space=pltpu.VMEM),
            scratch_shapes=[
                pltpu.VMEM((SLOTS, GROUP, tokens * heads, head), k.dtype),
                pltpu.VMEM((SLOTS, GROUP, tokens * heads, head), v.dtype),
                pltpu.VMEM((steps, inner, rows, head), jnp.bfloat16),
                pltpu.VMEM((steps, inner, 2, 128), jnp.float32),
                pltpu.VMEM((steps, outer, rows, head), jnp.bfloat16),
                pltpu.VMEM((steps, outer, 2, 128), jnp.float32),
                pltpu.SemaphoreType.DMA((SLOTS,)),
                pltpu.SemaphoreType.DMA((SLOTS,)),
                pltpu.SemaphoreType.DMA,
                pltpu.SemaphoreType.DMA,
                pltpu.SemaphoreType.DMA((steps,)),
                pltpu.SemaphoreType.DMA((steps,)),
                pltpu.SemaphoreType.DMA,
                pltpu.SemaphoreType.DMA,
                pltpu.SemaphoreType.DMA((steps,)),
                pltpu.SemaphoreType.DMA((steps,)),
            ],
            compiler_params=pltpu.CompilerParams(collective_id=0, has_side_effects=True, vmem_limit_bytes=60 * 2**20),
        )(q, k, v)
        return out.reshape(q.shape)

    return jax.shard_map(
        step,
        mesh=mesh,
        in_specs=(P("dp", None, None), P("dp", "sp", None, None), P("dp", "sp", None, None)),
        out_specs=P("dp", None, None),
        check_vma=False,
    )
```

```python
import jax
import jax.numpy as jnp
from jax import lax
from jax.experimental import pallas as pl
from jax.experimental.pallas import tpu as pltpu
from jax.sharding import PartitionSpec as P

MESH = pl.DeviceIdType.MESH
GROUP = 2
SLOTS = 8
GREET = 6
DIRECT = 0


def kernel(
    q_hbm, k_hbm, v_hbm, o_ref, q_ref, kbuf, vbuf, scores, mine, mine_stats, owned, owned_stats, direct, direct_stats, done,
    qsem, ksem, vsem, mine_sent, mine_stats_sent, owned_got, owned_stats_got, done_sent, done_got, direct_sent, direct_stats_sent, direct_got, direct_stats_got,
):
    batch, tokens, head = k_hbm.shape
    heads, n = q_ref.shape[1], owned.shape[0]
    steps, owners = batch // GROUP, mine.shape[0]
    last = owners // GROUP
    me, group = lax.axis_index("sp"), lax.axis_index("dp")
    my_seq = jnp.maximum(owners - 1 - me, 0)
    owner = me < owners

    def fetch(hbm, buf, sem, i):
        slot = lax.rem(i, SLOTS)
        return pltpu.make_async_copy(hbm.at[pl.ds(i * GROUP, GROUP)], buf.at[slot], sem.at[slot])

    def each(low, high, act):
        def body(i, _):
            act(i)
            return 0

        lax.fori_loop(low, high, body, 0)

    def prefetch(i):
        fetch(k_hbm, kbuf, ksem, i).start()
        fetch(v_hbm, vbuf, vsem, i).start()

    pltpu.make_async_copy(q_hbm, q_ref, qsem).start()
    each(0, min(SLOTS, steps), prefetch)

    def others(act):
        each(1, n, lambda j: act(lax.rem(me + j, n)))

    barrier = pltpu.get_barrier_semaphore()
    others(lambda peer: pl.semaphore_signal(barrier, inc=1, device_id=(group, peer), device_id_type=MESH))

    own = lax.rem(lax.broadcasted_iota(jnp.int32, (heads, tokens), 1), heads) == lax.broadcasted_iota(jnp.int32, (heads, tokens), 0)
    place = lax.broadcasted_iota(jnp.int32, (heads, 128), 1) - lax.broadcasted_iota(jnp.int32, (heads, 128), 0)
    eyes = [place == g * heads for g in range(GROUP)]

    def across(column, g=0):
        return jnp.sum(jnp.where(eyes[g], column, 0.0), 0, keepdims=True)

    def down(line, g=0):
        return jnp.sum(jnp.where(eyes[g], line, 0.0), 1, keepdims=True)

    def send(src, dst, sent, got, peer):
        pltpu.make_async_remote_copy(src_ref=src, dst_ref=dst, send_sem=sent, recv_sem=got, device_id=(group, peer), device_id_type=MESH).start()

    def wait(ref, sem):
        pltpu.make_async_copy(ref, ref, sem).wait()

    def score(i):
        slot = lax.rem(i, SLOTS)
        for g in range(GROUP):
            scores[lax.rem(i, 2), g] = lax.dot_general(q_ref[i * GROUP + g], kbuf[slot, g], (((1,), (1,)), ((), ())), preferred_element_type=jnp.float32)

    def attend(i, early):
        slot = lax.rem(i, SLOTS)
        highs, totals = [], []
        for g in range(GROUP):
            s = jnp.where(own, scores[lax.rem(i, 2), g] * head**-0.5, -jnp.inf)
            high = jnp.max(s, 1, keepdims=True)
            w = jnp.exp(s - high)
            total = jnp.sum(w, 1, keepdims=True)
            seen = jnp.dot(w.astype(jnp.bfloat16), vbuf[slot, g], preferred_element_type=jnp.float32).astype(jnp.bfloat16)
            if early:
                mine[i * GROUP + g] = seen
                mine_stats[i * GROUP + g] = jnp.concatenate([across(high), across(total)], 0)
            else:
                direct[i - last, me, g] = seen
                highs.append(across(high, g))
                totals.append(across(total, g))
        if not early:
            direct_stats[i - last, me] = jnp.concatenate([sum(highs), sum(totals)], 0)

    def to_owners(i):
        for g in range(GROUP):
            seq = i * GROUP + g
            to = owners - 1 - seq

            @pl.when(me != to)
            def _():
                send(mine.at[seq], owned.at[me], mine_sent, owned_got, to)
                send(mine_stats.at[seq], owned_stats.at[me], mine_stats_sent, owned_stats_got, to)

    def to_all(i):
        def both(peer):
            send(direct.at[i - last, me], direct.at[i - last, me], direct_sent, direct_got.at[i - last], peer)
            send(direct_stats.at[i - last, me], direct_stats.at[i - last, me], direct_stats_sent, direct_stats_got.at[i - last], peer)

        others(both)

    def merge(stats, parts):
        high = stats[:, 0, :]
        top = jnp.max(high, 0, keepdims=True)
        scale = jnp.exp(high - top)
        total = jnp.sum(stats[:, 1, :] * scale, 0, keepdims=True)
        outs = []
        for g, part in enumerate(parts):
            seen = sum(down(scale[s : s + 1], g) * part[s].astype(jnp.float32) for s in range(n))
            outs.append((seen / down(total, g)).astype(jnp.bfloat16))
        return outs

    def step(i, early, greeted=True, ahead=True):
        if ahead:
            fetch(k_hbm, kbuf, ksem, i + 1).wait()
        fetch(v_hbm, vbuf, vsem, i).wait()
        if ahead:
            score(i + 1)
        attend(i, early)
        if early and greeted:
            to_owners(i)
        if not early:
            to_all(i)
        if ahead:

            @pl.when(i + SLOTS < steps)
            def _():
                prefetch(i + SLOTS)

    wait(q_ref, qsem)
    fetch(k_hbm, kbuf, ksem, 0).wait()
    score(0)
    each(0, GREET, lambda i: step(i, True, greeted=False))
    pl.semaphore_wait(barrier, n - 1)
    each(0, GREET, to_owners)
    each(GREET, min(last, steps - 1), lambda i: step(i, True))
    each(last, steps - 1, lambda i: step(i, False))
    step(steps - 1, last == steps, ahead=False)

    @pl.when(owner)
    def _():
        wait(owned.at[pl.ds(0, n - 1)], owned_got)
        wait(owned_stats.at[pl.ds(0, n - 1)], owned_stats_got)
        owned[me] = mine[my_seq]
        owned_stats[me] = mine_stats[my_seq]
        done[my_seq] = merge(owned_stats, [owned])[0]
        others(lambda peer: send(done.at[my_seq], done.at[my_seq], done_sent, done_got, peer))

    for d in range(steps - last):
        wait(direct.at[d, pl.ds(0, n - 1)], direct_got.at[d])
        wait(direct_stats.at[d, pl.ds(0, n - 1)], direct_stats_got.at[d])
        outs = merge(direct_stats.at[d], [direct.at[d, :, g] for g in range(GROUP)])
        for g in range(GROUP):
            o_ref[owners + d * GROUP + g] = outs[g]

    def finish(count):
        wait(done.at[pl.ds(0, owners - count)], done_got)
        wait(mine.at[pl.ds(0, owners - count)], mine_sent)
        wait(mine_stats.at[pl.ds(0, owners - count)], mine_stats_sent)
        if count:
            wait(owned.at[pl.ds(0, n - 1)], done_sent)

    @pl.when(owner)
    def _():
        finish(1)

    if owners < n:

        @pl.when(jnp.logical_not(owner))
        def _():
            finish(0)

    o_ref[pl.ds(0, owners)] = done[...]
    if last < steps:
        wait(direct.at[:, pl.ds(0, n - 1)], direct_sent)
        wait(direct_stats.at[:, pl.ds(0, n - 1)], direct_stats_sent)


def solution(mesh):
    n = mesh.shape["sp"]

    def step(q, k, v):
        batch, tokens, heads, head = k.shape
        owners, late = batch - DIRECT * GROUP, max(DIRECT, 1)
        k, v = (a.reshape(batch, tokens * heads, head) for a in (k, v))
        dma = pltpu.SemaphoreType.DMA
        return pl.pallas_call(
            kernel,
            out_shape=jax.ShapeDtypeStruct(q.shape, q.dtype),
            in_specs=[pl.BlockSpec(memory_space=pltpu.HBM)] * 3,
            out_specs=pl.BlockSpec(memory_space=pltpu.VMEM),
            scratch_shapes=[
                pltpu.VMEM(q.shape, q.dtype),
                pltpu.VMEM((SLOTS, GROUP, tokens * heads, head), k.dtype),
                pltpu.VMEM((SLOTS, GROUP, tokens * heads, head), v.dtype),
                pltpu.VMEM((2, GROUP, heads, tokens * heads), jnp.float32),
                pltpu.VMEM((owners, heads, head), jnp.bfloat16),
                pltpu.VMEM((owners, 2, 128), jnp.float32),
                pltpu.VMEM((n, heads, head), jnp.bfloat16),
                pltpu.VMEM((n, 2, 128), jnp.float32),
                pltpu.VMEM((late, n, GROUP, heads, head), jnp.bfloat16),
                pltpu.VMEM((late, n, 2, 128), jnp.float32),
                pltpu.VMEM((owners, heads, head), jnp.bfloat16),
                dma, dma((SLOTS,)), dma((SLOTS,)), dma, dma, dma, dma, dma, dma, dma, dma, dma((late,)), dma((late,)),
            ],
            compiler_params=pltpu.CompilerParams(collective_id=0, has_side_effects=True, vmem_limit_bytes=40 * 2**20),
        )(pltpu.with_memory_space_constraint(q, pltpu.HBM), k, v)

    return jax.shard_map(
        step,
        mesh=mesh,
        in_specs=(P("dp", None, None), P("dp", "sp", None, None), P("dp", "sp", None, None)),
        out_specs=P("dp", None, None),
        check_vma=False,
    )
```

```python
import jax
import jax.numpy as jnp
from jax import lax
from jax.experimental import pallas as pl
from jax.experimental.pallas import tpu as pltpu
from jax.sharding import PartitionSpec as P

MESH = pl.DeviceIdType.MESH
GROUP = 2
SLOTS = 8
GREET = 6


def kernel(
    q_hbm, k_hbm, v_hbm, o_ref, q_ref, kbuf, vbuf, scores, mine, mine_stats, owned, owned_stats, direct, direct_stats, done,
    qsem, ksem, vsem, mine_sent, mine_stats_sent, owned_got, owned_stats_got, done_sent, done_got, direct_sent, direct_stats_sent, direct_got, direct_stats_got,
):
    batch, tokens, head = k_hbm.shape
    heads, n = q_ref.shape[1], owned.shape[0]
    steps, owners = batch // GROUP, done.shape[0]
    me, group = lax.axis_index("sp"), lax.axis_index("dp")
    my_step = owners - 1 - me
    owner = my_step >= 0

    def fetch(hbm, buf, sem, i):
        slot = lax.rem(i, SLOTS)
        return pltpu.make_async_copy(hbm.at[pl.ds(i * GROUP, GROUP)], buf.at[slot], sem.at[slot])

    def values(i, g):
        slot = lax.rem(i, SLOTS)
        return pltpu.make_async_copy(v_hbm.at[i * GROUP + g], vbuf.at[slot, g], vsem.at[slot, g])

    def each(low, high, act):
        def body(i, _):
            act(i)
            return 0

        lax.fori_loop(low, high, body, 0)

    def prefetch(i):
        fetch(k_hbm, kbuf, ksem, i).start()
        for g in range(GROUP):
            values(i, g).start()

    pltpu.make_async_copy(q_hbm, q_ref, qsem).start()
    each(0, min(SLOTS, steps), prefetch)

    def others(act):
        each(0, n - 1, lambda j: act(j + (j >= me).astype(jnp.int32)))

    barrier = pltpu.get_barrier_semaphore()
    others(lambda peer: pl.semaphore_signal(barrier, inc=1, device_id=(group, peer), device_id_type=MESH))

    own = lax.rem(lax.broadcasted_iota(jnp.int32, (heads, tokens), 1), heads) == lax.broadcasted_iota(jnp.int32, (heads, tokens), 0)
    place = lax.broadcasted_iota(jnp.int32, (heads, 128), 1) - lax.broadcasted_iota(jnp.int32, (heads, 128), 0)
    eyes = [place == g * heads for g in range(GROUP)]

    def across(column, g=0):
        return jnp.sum(jnp.where(eyes[g], column, 0.0), 0, keepdims=True)

    def down(line, g=0):
        return jnp.sum(jnp.where(eyes[g], line, 0.0), 1, keepdims=True)

    def send(src, dst, sent, got, peer):
        pltpu.make_async_remote_copy(src_ref=src, dst_ref=dst, send_sem=sent, recv_sem=got, device_id=(group, peer), device_id_type=MESH).start()

    def wait(ref, sem):
        pltpu.make_async_copy(ref, ref, sem).wait()

    def score(i):
        slot = lax.rem(i, SLOTS)
        for g in range(GROUP):
            scores[lax.rem(i, 2), g] = lax.dot_general(q_ref[i * GROUP + g], kbuf[slot, g], (((1,), (1,)), ((), ())), preferred_element_type=jnp.float32)

    def attend(i, final):
        slot = lax.rem(i, SLOTS)
        weights, highs, totals = [], [], []
        for g in range(GROUP):
            s = jnp.where(own, scores[lax.rem(i, 2), g] * head**-0.5, -jnp.inf)
            high = jnp.max(s, 1, keepdims=True)
            w = jnp.exp(s - high)
            weights.append(w.astype(jnp.bfloat16))
            highs.append(across(high, g))
            totals.append(across(jnp.sum(w, 1, keepdims=True), g))
        stats = jnp.concatenate([sum(highs), sum(totals)], 0)
        if final:
            direct_stats[me] = stats
        else:
            mine_stats[i] = stats
        for g in range(GROUP):
            if final:
                values(i, g).wait()
            seen = jnp.dot(weights[g], vbuf[slot, g], preferred_element_type=jnp.float32).astype(jnp.bfloat16)
            if final:
                direct[me, g] = seen
            else:
                mine[i, g] = seen

    def to_all():
        def both(peer):
            send(direct.at[me], direct.at[me], direct_sent, direct_got, peer)
            send(direct_stats.at[me], direct_stats.at[me], direct_stats_sent, direct_stats_got, peer)

        others(both)

    def to_owner(i):
        to = owners - 1 - i

        @pl.when(me != to)
        def _():
            send(mine.at[i], owned.at[me], mine_sent, owned_got, to)
            send(mine_stats.at[i], owned_stats.at[me], mine_stats_sent, owned_stats_got, to)

    def merge(stats, parts):
        high = stats[:, 0, :]
        top = jnp.max(high, 0, keepdims=True)
        scale = jnp.exp(high - top)
        total = jnp.sum(stats[:, 1, :] * scale, 0, keepdims=True)
        outs = []
        for g in range(GROUP):
            seen = sum(down(scale[s : s + 1], g) * parts[s, g].astype(jnp.float32) for s in range(n))
            outs.append((seen / down(total, g)).astype(jnp.bfloat16))
        return jnp.stack(outs)

    def step(i, greeted):
        fetch(k_hbm, kbuf, ksem, i + 1).wait()
        for g in range(GROUP):
            values(i, g).wait()
        score(i + 1)
        attend(i, False)
        if greeted:
            to_owner(i)

        @pl.when(i + SLOTS < steps)
        def _():
            prefetch(i + SLOTS)

    wait(q_ref, qsem)
    fetch(k_hbm, kbuf, ksem, 0).wait()
    score(0)
    each(0, GREET, lambda i: step(i, False))
    pl.semaphore_wait(barrier, n - 1)
    each(0, GREET, to_owner)
    each(GREET, steps - 1, lambda i: step(i, True))
    attend(steps - 1, True)
    to_all()

    @pl.when(owner)
    def _():
        wait(owned.at[pl.ds(0, n - 1)], owned_got)
        wait(owned_stats.at[pl.ds(0, n - 1)], owned_stats_got)
        owned[me] = mine[my_step]
        owned_stats[me] = mine_stats[my_step]
        done[my_step] = merge(owned_stats, owned)
        others(lambda peer: send(done.at[my_step], done.at[my_step], done_sent, done_got, peer))

    wait(direct.at[pl.ds(0, n - 1)], direct_got)
    wait(direct_stats.at[pl.ds(0, n - 1)], direct_stats_got)
    o_ref[pl.ds(owners * GROUP, GROUP)] = merge(direct_stats, direct)

    def finish(count):
        wait(done.at[pl.ds(0, owners - count)], done_got)
        wait(mine.at[pl.ds(0, owners - count)], mine_sent)
        wait(mine_stats.at[pl.ds(0, owners - count)], mine_stats_sent)
        if count:
            wait(owned.at[pl.ds(0, n - 1)], done_sent)

    @pl.when(owner)
    def _():
        finish(1)

    @pl.when(jnp.logical_not(owner))
    def _():
        finish(0)

    o_ref[pl.ds(0, owners * GROUP)] = done[...].reshape(owners * GROUP, heads, head)
    wait(direct.at[pl.ds(0, n - 1)], direct_sent)
    wait(direct_stats.at[pl.ds(0, n - 1)], direct_stats_sent)


def solution(mesh):
    n = mesh.shape["sp"]

    def step(q, k, v):
        batch, tokens, heads, head = k.shape
        owners = batch // GROUP - 1
        k, v = (a.reshape(batch, tokens * heads, head) for a in (k, v))
        dma = pltpu.SemaphoreType.DMA
        return pl.pallas_call(
            kernel,
            out_shape=jax.ShapeDtypeStruct(q.shape, q.dtype),
            in_specs=[pl.BlockSpec(memory_space=pltpu.HBM)] * 3,
            out_specs=pl.BlockSpec(memory_space=pltpu.VMEM),
            scratch_shapes=[
                pltpu.VMEM(q.shape, q.dtype),
                pltpu.VMEM((SLOTS, GROUP, tokens * heads, head), k.dtype),
                pltpu.VMEM((SLOTS, GROUP, tokens * heads, head), v.dtype),
                pltpu.VMEM((2, GROUP, heads, tokens * heads), jnp.float32),
                pltpu.VMEM((owners, GROUP, heads, head), jnp.bfloat16),
                pltpu.VMEM((owners, 2, 128), jnp.float32),
                pltpu.VMEM((n, GROUP, heads, head), jnp.bfloat16),
                pltpu.VMEM((n, 2, 128), jnp.float32),
                pltpu.VMEM((n, GROUP, heads, head), jnp.bfloat16),
                pltpu.VMEM((n, 2, 128), jnp.float32),
                pltpu.VMEM((owners, GROUP, heads, head), jnp.bfloat16),
                dma, dma((SLOTS,)), dma((SLOTS, GROUP)), dma, dma, dma, dma, dma, dma, dma, dma, dma, dma,
            ],
            compiler_params=pltpu.CompilerParams(collective_id=0, has_side_effects=True, vmem_limit_bytes=40 * 2**20),
        )(pltpu.with_memory_space_constraint(q, pltpu.HBM), k, v)

    return jax.shard_map(
        step,
        mesh=mesh,
        in_specs=(P("dp", None, None), P("dp", "sp", None, None), P("dp", "sp", None, None)),
        out_specs=P("dp", None, None),
        check_vma=False,
    )
```

```python
import math

import jax
import jax.numpy as jnp
from jax import lax
from jax.experimental import pallas as pl
from jax.experimental.pallas import tpu as pltpu
from jax.sharding import PartitionSpec as P

MESH = pl.DeviceIdType.MESH
CORES = 2
GROUP = 2
SLOTS = 4
GREET = 6


def kernel(
    q_hbm, k_hbm, v_hbm, o_ref, q_ref, kbuf, vbuf, scores, mine, mine_stats, owned, owned_stats, done,
    qsem, ksem, vsem, mine_sent, mine_stats_sent, owned_got, owned_stats_got, done_sent, done_got,
):
    batch, tokens, head = k_hbm.shape
    heads, n = q_ref.shape[1], owned.shape[0]
    steps, owners = batch // GROUP, done.shape[0]
    outer = math.isqrt(n // CORES)
    inner = n // outer
    me, group = lax.axis_index("sp"), lax.axis_index("dp")
    my_step = owners - 1 - me
    owner = my_step >= 0

    def fetch(hbm, buf, sem, i):
        slot = lax.rem(i, SLOTS)
        return pltpu.make_async_copy(hbm.at[pl.ds(i * GROUP, GROUP)], buf.at[slot], sem.at[slot])

    def each(low, high, act):
        def body(i, _):
            act(i)
            return 0

        lax.fori_loop(low, high, body, 0)

    def prefetch(i):
        @pl.when(i + 1 < steps)
        def _():
            fetch(k_hbm, kbuf, ksem, i + 1).start()

        @pl.when(i < steps)
        def _():
            fetch(v_hbm, vbuf, vsem, i).start()

    pltpu.make_async_copy(q_hbm, q_ref, qsem).start()
    fetch(k_hbm, kbuf, ksem, 0).start()
    each(0, SLOTS - 1, prefetch)

    def others(act):
        each(0, n - 1, lambda j: act(j + (j >= me).astype(jnp.int32)))

    barrier = pltpu.get_barrier_semaphore()
    others(lambda peer: pl.semaphore_signal(barrier, inc=1, device_id=(group, peer), device_id_type=MESH))

    own = lax.rem(lax.broadcasted_iota(jnp.int32, (heads, tokens), 1), heads) == lax.broadcasted_iota(jnp.int32, (heads, tokens), 0)
    place = lax.broadcasted_iota(jnp.int32, (heads, 128), 1) - lax.broadcasted_iota(jnp.int32, (heads, 128), 0)
    eyes = [place == g * heads for g in range(GROUP)]

    def across(column, g=0):
        return jnp.sum(jnp.where(eyes[g], column, 0.0), 0, keepdims=True)

    def down(line, g=0):
        return jnp.sum(jnp.where(eyes[g], line, 0.0), 1, keepdims=True)

    def send(src, dst, sent, got, peer):
        pltpu.make_async_remote_copy(src_ref=src, dst_ref=dst, send_sem=sent, recv_sem=got, device_id=(group, peer), device_id_type=MESH).start()

    def wait(ref, sem):
        pltpu.make_async_copy(ref, ref, sem).wait()

    def score(i):
        slot = lax.rem(i, SLOTS)
        for g in range(GROUP):
            scores[lax.rem(i, 2), g] = lax.dot_general(q_ref[i * GROUP + g], kbuf[slot, g], (((1,), (1,)), ((), ())), preferred_element_type=jnp.float32)

    def weigh(i):
        weights, highs, totals = [], [], []
        for g in range(GROUP):
            s = jnp.where(own, scores[lax.rem(i, 2), g] * head**-0.5, -jnp.inf)
            high = jnp.max(s, 1, keepdims=True)
            w = jnp.exp(s - high)
            weights.append(w.astype(jnp.bfloat16))
            highs.append(across(high, g))
            totals.append(across(jnp.sum(w, 1, keepdims=True), g))
        return weights, jnp.concatenate([sum(highs), sum(totals)], 0)

    def see(i, weights, part):
        slot = lax.rem(i, SLOTS)
        for g in range(GROUP):
            part[g] = jnp.dot(weights[g], vbuf[slot, g], preferred_element_type=jnp.float32).astype(jnp.bfloat16)

    def attend(i):
        weights, mine_stats[i] = weigh(i)
        see(i, weights, mine.at[i])

    def to_owner(i):
        to = owners - 1 - i

        @pl.when(me != to)
        def _():
            send(mine.at[i], owned.at[me], mine_sent, owned_got, to)
            send(mine_stats.at[i], owned_stats.at[me], mine_stats_sent, owned_stats_got, to)

    def merge(stats, parts):
        high = stats[:, 0, :]
        top = jnp.max(high, 0, keepdims=True)
        scale = jnp.exp(high - top)
        total = jnp.sum(stats[:, 1, :] * scale, 0, keepdims=True)
        outs = []
        for g in range(GROUP):
            seen = sum(down(scale[s : s + 1], g) * parts[s, g].astype(jnp.float32) for s in range(n))
            outs.append((seen / down(total, g)).astype(jnp.bfloat16))
        return jnp.stack(outs)

    def step(i):
        @pl.when(i == GREET)
        def _():
            pl.semaphore_wait(barrier, n - 1)
            each(0, GREET, to_owner)

        fetch(k_hbm, kbuf, ksem, i + 1).wait()
        fetch(v_hbm, vbuf, vsem, i).wait()
        attend(i)
        score(i + 1)
        pl.when(i >= GREET)(lambda: to_owner(i))
        prefetch(i + SLOTS)

    wait(q_ref, qsem)
    fetch(k_hbm, kbuf, ksem, 0).wait()
    score(0)
    prefetch(SLOTS - 1)
    each(0, steps - 2, step)
    fetch(k_hbm, kbuf, ksem, steps - 1).wait()
    score(steps - 1)
    fetch(v_hbm, vbuf, vsem, steps - 2).wait()
    attend(steps - 2)
    weights, mine_stats[steps - 1] = weigh(steps - 1)
    to_owner(steps - 2)
    fetch(v_hbm, vbuf, vsem, steps - 1).wait()
    see(steps - 1, weights, mine.at[steps - 1])
    to_owner(steps - 1)

    @pl.when(owner)
    def _():
        wait(owned.at[pl.ds(0, n - 1)], owned_got)
        wait(owned_stats.at[pl.ds(0, n - 1)], owned_stats_got)
        owned[me] = mine[my_step]
        owned_stats[me] = mine_stats[my_step]
        done[my_step] = merge(owned_stats, owned)
        row, rest = lax.div(me, inner), lax.rem(me, inner)
        turn = (lax.div(rest, CORES) * outer + row) * CORES + lax.rem(rest, CORES)

        def tell(j):
            k = j + (j >= turn).astype(jnp.int32)
            peer = lax.rem(lax.div(k, CORES), outer) * inner + lax.div(k, CORES * outer) * CORES + lax.rem(k, CORES)
            send(done.at[my_step], done.at[my_step], done_sent, done_got, peer)

        each(0, n - 1, tell)

    def finish(count):
        wait(done.at[pl.ds(0, owners - count)], done_got)
        wait(mine.at[pl.ds(0, owners - count)], mine_sent)
        wait(mine_stats.at[pl.ds(0, owners - count)], mine_stats_sent)
        if count:
            wait(owned.at[pl.ds(0, n - 1)], done_sent)

    @pl.when(owner)
    def _():
        finish(1)

    @pl.when(jnp.logical_not(owner))
    def _():
        finish(0)

    o_ref[...] = done[...].reshape(batch, heads, head)


def solution(mesh):
    n = mesh.shape["sp"]

    def step(q, k, v):
        batch, tokens, heads, head = k.shape
        owners = batch // GROUP
        k, v = (a.reshape(batch, tokens * heads, head) for a in (k, v))
        dma = pltpu.SemaphoreType.DMA
        return pl.pallas_call(
            kernel,
            out_shape=jax.ShapeDtypeStruct(q.shape, q.dtype),
            in_specs=[pl.BlockSpec(memory_space=pltpu.HBM)] * 3,
            out_specs=pl.BlockSpec(memory_space=pltpu.VMEM),
            scratch_shapes=[
                pltpu.VMEM(q.shape, q.dtype),
                pltpu.VMEM((SLOTS, GROUP, tokens * heads, head), k.dtype),
                pltpu.VMEM((SLOTS, GROUP, tokens * heads, head), v.dtype),
                pltpu.VMEM((2, GROUP, heads, tokens * heads), jnp.float32),
                pltpu.VMEM((owners, GROUP, heads, head), jnp.bfloat16),
                pltpu.VMEM((owners, 2, 128), jnp.float32),
                pltpu.VMEM((n, GROUP, heads, head), jnp.bfloat16),
                pltpu.VMEM((n, 2, 128), jnp.float32),
                pltpu.VMEM((owners, GROUP, heads, head), jnp.bfloat16),
                dma, dma((SLOTS,)), dma((SLOTS,)), dma, dma, dma, dma, dma, dma,
            ],
            compiler_params=pltpu.CompilerParams(collective_id=0, has_side_effects=True, vmem_limit_bytes=24 * 2**20),
        )(pltpu.with_memory_space_constraint(q, pltpu.HBM), k, v)

    return jax.shard_map(
        step,
        mesh=mesh,
        in_specs=(P("dp", None, None), P("dp", "sp", None, None), P("dp", "sp", None, None)),
        out_specs=P("dp", None, None),
        check_vma=False,
    )
```

```python
import math

import jax
import jax.numpy as jnp
from jax import lax
from jax.experimental import pallas as pl
from jax.experimental.pallas import tpu as pltpu
from jax.sharding import PartitionSpec as P

MESH = pl.DeviceIdType.MESH
CORES = 2
GROUP = 2
SLOTS = 3
GREET = 6


def kernel(
    q_hbm, k_hbm, v_hbm, o_ref, q_ref, kbuf, vbuf, scores, mine, mine_stats, owned, owned_stats, done,
    qsem, ksem, vsem, mine_sent, mine_stats_sent, owned_got, owned_stats_got, done_sent, done_got,
):
    batch, tokens, head = k_hbm.shape
    heads, n = q_ref.shape[1], owned.shape[0]
    steps, owners = batch // GROUP, done.shape[0]
    outer = math.isqrt(n // CORES)
    inner = n // outer
    me, group = lax.axis_index("sp"), lax.axis_index("dp")
    my_step = owners - 1 - me
    owner = my_step >= 0

    def fetch(hbm, buf, sem, i):
        slot = lax.rem(i, SLOTS)
        return pltpu.make_async_copy(hbm.at[pl.ds(i * GROUP, GROUP)], buf.at[slot], sem.at[slot])

    def each(low, high, act):
        def body(i, _):
            act(i)
            return 0

        lax.fori_loop(low, high, body, 0)

    def prefetch(i):
        @pl.when(i + 1 < steps)
        def _():
            fetch(k_hbm, kbuf, ksem, i + 1).start()

        @pl.when(i < steps)
        def _():
            fetch(v_hbm, vbuf, vsem, i).start()

    pltpu.make_async_copy(q_hbm, q_ref, qsem).start()
    fetch(k_hbm, kbuf, ksem, 0).start()
    each(0, SLOTS - 1, prefetch)

    def others(act):
        each(0, n - 1, lambda j: act(j + (j >= me).astype(jnp.int32)))

    barrier = pltpu.get_barrier_semaphore()
    others(lambda peer: pl.semaphore_signal(barrier, inc=1, device_id=(group, peer), device_id_type=MESH))

    own = lax.rem(lax.broadcasted_iota(jnp.int32, (heads, tokens), 1), heads) == lax.broadcasted_iota(jnp.int32, (heads, tokens), 0)
    place = lax.broadcasted_iota(jnp.int32, (heads, 128), 1) - lax.broadcasted_iota(jnp.int32, (heads, 128), 0)
    eyes = [place == g * heads for g in range(GROUP)]

    def across(column, g=0):
        return jnp.sum(jnp.where(eyes[g], column, 0.0), 0, keepdims=True)

    def down(line, g=0):
        return jnp.sum(jnp.where(eyes[g], line, 0.0), 1, keepdims=True)

    def send(src, dst, sent, got, peer):
        pltpu.make_async_remote_copy(src_ref=src, dst_ref=dst, send_sem=sent, recv_sem=got, device_id=(group, peer), device_id_type=MESH).start()

    def wait(ref, sem):
        pltpu.make_async_copy(ref, ref, sem).wait()

    def score(i):
        slot = lax.rem(i, SLOTS)
        for g in range(GROUP):
            scores[lax.rem(i, 2), g] = lax.dot_general(q_ref[i * GROUP + g], kbuf[slot, g], (((1,), (1,)), ((), ())), preferred_element_type=jnp.float32)

    def weigh(i):
        weights, highs, totals = [], [], []
        for g in range(GROUP):
            s = jnp.where(own, scores[lax.rem(i, 2), g] * head**-0.5, -jnp.inf)
            high = jnp.max(s, 1, keepdims=True)
            w = jnp.exp(s - high)
            weights.append(w.astype(jnp.bfloat16))
            highs.append(across(high, g))
            totals.append(across(jnp.sum(w, 1, keepdims=True), g))
        return weights, jnp.concatenate([sum(highs), sum(totals)], 0)

    def see(i, weights, part):
        slot = lax.rem(i, SLOTS)
        for g in range(GROUP):
            part[g] = jnp.dot(weights[g], vbuf[slot, g], preferred_element_type=jnp.float32).astype(jnp.bfloat16)

    def attend(i):
        weights, mine_stats[i] = weigh(i)
        see(i, weights, mine.at[i])

    def to_owner(i):
        to = owners - 1 - i

        @pl.when(me != to)
        def _():
            send(mine.at[i], owned.at[me], mine_sent, owned_got, to)
            send(mine_stats.at[i], owned_stats.at[me], mine_stats_sent, owned_stats_got, to)

    def merge(stats, parts):
        high = stats[:, 0, :]
        top = jnp.max(high, 0, keepdims=True)
        scale = jnp.exp(high - top)
        total = jnp.sum(stats[:, 1, :] * scale, 0, keepdims=True)
        outs = []
        for g in range(GROUP):
            seen = sum(down(scale[s : s + 1], g) * parts[s, g].astype(jnp.float32) for s in range(n))
            outs.append((seen / down(total, g)).astype(jnp.bfloat16))
        return jnp.stack(outs)

    def step(i):
        @pl.when(i == GREET)
        def _():
            pl.semaphore_wait(barrier, n - 1)
            each(0, GREET, to_owner)

        fetch(k_hbm, kbuf, ksem, i + 1).wait()
        fetch(v_hbm, vbuf, vsem, i).wait()
        attend(i)
        score(i + 1)
        pl.when(i >= GREET)(lambda: to_owner(i))
        prefetch(i + SLOTS)

    wait(q_ref, qsem)
    fetch(k_hbm, kbuf, ksem, 0).wait()
    score(0)
    prefetch(SLOTS - 1)
    each(0, steps - 2, step)
    fetch(k_hbm, kbuf, ksem, steps - 1).wait()
    score(steps - 1)
    fetch(v_hbm, vbuf, vsem, steps - 2).wait()
    attend(steps - 2)
    weights, mine_stats[steps - 1] = weigh(steps - 1)
    to_owner(steps - 2)
    fetch(v_hbm, vbuf, vsem, steps - 1).wait()
    see(steps - 1, weights, mine.at[steps - 1])
    to_owner(steps - 1)

    @pl.when(owner)
    def _():
        wait(owned.at[pl.ds(0, n - 1)], owned_got)
        wait(owned_stats.at[pl.ds(0, n - 1)], owned_stats_got)
        owned[me] = mine[my_step]
        owned_stats[me] = mine_stats[my_step]
        done[my_step] = merge(owned_stats, owned)
        row, rest = lax.div(me, inner), lax.rem(me, inner)
        turn = (lax.div(rest, CORES) * outer + row) * CORES + lax.rem(rest, CORES)
        for j in range(n - 1):
            k = j + (j >= turn).astype(jnp.int32)
            peer = lax.rem(lax.div(k, CORES), outer) * inner + lax.div(k, CORES * outer) * CORES + lax.rem(k, CORES)
            send(done.at[my_step], done.at[my_step], done_sent, done_got, peer)

    def finish(count):
        wait(done.at[pl.ds(0, owners - count)], done_got)
        wait(mine.at[pl.ds(0, owners - count)], mine_sent)
        wait(mine_stats.at[pl.ds(0, owners - count)], mine_stats_sent)
        if count:
            wait(owned.at[pl.ds(0, n - 1)], done_sent)

    @pl.when(owner)
    def _():
        finish(1)

    @pl.when(jnp.logical_not(owner))
    def _():
        finish(0)

    o_ref[...] = done[...].reshape(batch, heads, head)


def solution(mesh):
    n = mesh.shape["sp"]

    def step(q, k, v):
        batch, tokens, heads, head = k.shape
        owners = batch // GROUP
        k, v = (a.reshape(batch, tokens * heads, head) for a in (k, v))
        dma = pltpu.SemaphoreType.DMA
        return pl.pallas_call(
            kernel,
            out_shape=jax.ShapeDtypeStruct(q.shape, q.dtype),
            in_specs=[pl.BlockSpec(memory_space=pltpu.HBM)] * 3,
            out_specs=pl.BlockSpec(memory_space=pltpu.VMEM),
            scratch_shapes=[
                pltpu.VMEM(q.shape, q.dtype),
                pltpu.VMEM((SLOTS, GROUP, tokens * heads, head), k.dtype),
                pltpu.VMEM((SLOTS, GROUP, tokens * heads, head), v.dtype),
                pltpu.VMEM((2, GROUP, heads, tokens * heads), jnp.float32),
                pltpu.VMEM((owners, GROUP, heads, head), jnp.bfloat16),
                pltpu.VMEM((owners, 2, 128), jnp.float32),
                pltpu.VMEM((n, GROUP, heads, head), jnp.bfloat16),
                pltpu.VMEM((n, 2, 128), jnp.float32),
                pltpu.VMEM((owners, GROUP, heads, head), jnp.bfloat16),
                dma, dma((SLOTS,)), dma((SLOTS,)), dma, dma, dma, dma, dma, dma,
            ],
            compiler_params=pltpu.CompilerParams(collective_id=0, has_side_effects=True, vmem_limit_bytes=24 * 2**20),
        )(pltpu.with_memory_space_constraint(q, pltpu.HBM), k, v)

    return jax.shard_map(
        step,
        mesh=mesh,
        in_specs=(P("dp", None, None), P("dp", "sp", None, None), P("dp", "sp", None, None)),
        out_specs=P("dp", None, None),
        check_vma=False,
    )
```
